32 devices in a mesh: section: 2 (over core), expert: 16 (over z, y, x).
Axes of the slice: x: 2, y: 2, z: 4, core: 2. Of those that a mesh axis runs over, the one named last changes fastest.
Arguments:
- grad_out: bfloat16 [2, 2048, 4096], P('section', 'expert'), may hold values from -6 to 6
- saved_hidden: bfloat16 [2, 2048, 8, 1024], P('section', 'expert'), may hold values from -6 to 6
- routes: int32 [2, 2048, 8], P('section', 'expert'), may hold values from 0 to 15, all different within a row; in each aligned block of 128 rows (0 to 127, 128 to 255, ..., all dimensions but the last counted through in order) at most 96 rows name the same one
- scores: float32 [2, 2048, 8], P('section', 'expert'), may hold values from 0.02 to 0.98
- down_weight: bfloat16 [2, 16, 1024, 4096], P('section', 'expert'), may hold values from -0.1875 to 0.1875
- router: bfloat16 [2, 16, 4096], P('section'), may hold values from -0.59765625 to 0.59765625
Outputs:
- weight_grad: bfloat16 [2, 16, 1024, 4096], P('section', 'expert')
- handed: bfloat16 [2, 2048, 4096], P('section', 'expert')
The draws below stay inside these ranges and needn't reach their ends.
Inputs may be any that keep to these rules, and one draw needn't show every extreme that they name: `routes`: each token names 8 different experts. Among the 128 tokens of one index of expert (aligned blocks), no expert is named more than 96 times, and in every draw some expert is named exactly 96 times in some block.
All inputs are finite; a program needn't handle non-finite values.
Results may differ from the reference program's by a relative error of at most 0.007.
Values may be sent and summed in bfloat16 or wider, within the bound.
No kernel may reach another device: no remote copies, remote signals or barrier semaphores. Data moves between devices by JAX's collectives and lax.ppermute only.
A program may use at most 128 MiB of HBM per device.

```python
import math
import jax
import jax.numpy as jnp
import numpy as np
from jax import lax

D = 4096
FF = 1024
TOP = 8
TOK_DEV = 128
SECTIONS = 2
EXPERTS = 16
TOKENS = 2048
CAP = 96


def levels(stream_key, dims, shards, smallest, high):
    gain, own = 1.0, jax.random.fold_in(stream_key, 6)
    for axis_at, shards_of in shards:
        heights = jnp.exp(jax.random.uniform(jax.random.fold_in(own, axis_at), (shards_of,), jnp.float32, smallest / len(shards), high / len(shards)))
        gain = gain * jnp.repeat(heights, dims[axis_at] // shards_of).reshape([-1 if axis == axis_at else 1 for axis in range(len(dims))])
    return gain


def deal_out(stream_key, own, number, rows, amount, top, bound, skew):
    sequence = jax.random.permutation(stream_key, amount)
    packed, ordinary = load_shares(amount, rows * top, bound, skew, True), load_shares(amount, rows * top, bound, skew, False)
    places = jnp.arange(amount)

    def named(lengths, offset_by):
        used = int((lengths > 0).sum())
        fixed = max(1, used // 4)
        moved = fixed + (places - fixed + offset_by * (used - fixed)) % max(1, amount - fixed)
        return jnp.zeros((amount,), jnp.int32).at[sequence[jnp.where(places < fixed, places, moved)]].set(jnp.asarray(lengths, jnp.int32))

    lengths = jnp.where(number % 4 == 0, named(packed, number // 4), named(ordinary, number - number // 4 - 1))
    mixed = jax.random.permutation(jax.random.fold_in(own, 3), amount)
    source_of, sink = mixed[0:amount // 2 * 2:2], mixed[1:amount // 2 * 2:2]
    room = jnp.minimum(lengths[source_of] - 1, bound - lengths[sink]) // 2
    room = jnp.where((source_of == sequence[0]) | (sink == sequence[0]) | (lengths[sink] == 0), 0, jnp.maximum(room, 0))
    moved = jax.random.randint(jax.random.fold_in(own, 4), (amount // 2,), 0, 1 << 20) % (room + 1)
    lengths = lengths.at[source_of].add(-moved).at[sink].add(moved)
    items = jnp.searchsorted(jnp.cumsum(lengths), jnp.arange(rows * top), side="right").astype(jnp.int32)
    table = items.reshape(top, rows).T
    table = table[jax.random.permutation(jax.random.fold_in(own, 1), rows)]
    offset_by = jax.random.randint(jax.random.fold_in(own, 2), (rows, 1), 0, top)
    return jnp.take_along_axis(table, (jnp.arange(top)[None, :] + offset_by) % top, axis=1)


def load_shares(count, total, most, slope, full):
    portions = [(1 << 20) // math.isqrt(grade ** slope) + 1 for grade in range(1, count + 1)]
    largest = most if full else min(most, max(-(-total // count), total * portions[0] // sum(portions)))
    least = 1 if total - largest >= count - 1 else 0
    holding, rest = [largest] + [least] * (count - 1), total - largest - least * (count - 1)
    while rest > 0:
        free = [i for i in range(1, count) if holding[i] < largest] or [i for i in range(1, count) if holding[i] < most]
        mass, budget = sum([portions[i] for i in free]), rest
        for i in free:
            extra = min(most - holding[i], max(1, budget * portions[i] // mass), rest)
            holding[i] = holding[i] + extra
            rest = rest - extra
    return np.array(holding)


def centred(own_key, extent, width, most, shards=(), kind=jnp.bfloat16):
    result = jax.random.normal(own_key, extent, jnp.float32) * width
    if len(shards) > 0:
        result = levels(own_key, extent, shards, -0.22, 0.18) * result
    return jnp.clip(result, min=-most, max=most).astype(kind)


def setup_inputs(seed: int = 0) -> dict:
    key_of = jax.random.split(jax.random.key(seed), 7)
    grad_out = centred(key_of[0], (SECTIONS, TOKENS, D), 1.0, 6.0, ((0, 2), (1, 16)))
    saved_hidden = centred(key_of[1], (SECTIONS, TOKENS, TOP, FF), 1.0, 6.0, ((0, 2), (1, 16)))
    routes_keys = jax.random.split(jax.random.fold_in(key_of[2], 1), SECTIONS * TOKENS // TOK_DEV)
    routes_turns = jax.random.permutation(jax.random.fold_in(key_of[2], 3), SECTIONS * TOKENS // TOK_DEV)
    routes = jax.vmap(lambda own, number: deal_out(jax.random.fold_in(key_of[2], 2), own, number, TOK_DEV, EXPERTS, TOP, CAP, 2))(routes_keys, routes_turns).reshape((SECTIONS, TOKENS, TOP))
    scores = jnp.clip(0.02 + 0.96000002 * jax.random.uniform(key_of[3], (SECTIONS, TOKENS, TOP), jnp.float32) ** levels(key_of[3], (SECTIONS, TOKENS, TOP), ((0, 2), (1, 16)), -0.2, 0.2), 0.02, 0.98)
    down_weight = centred(key_of[4], (SECTIONS, EXPERTS, FF, D), FF ** -0.5, 0.1875, ((0, 2), (1, 16)))
    router = centred(key_of[5], (SECTIONS, EXPERTS, D), 0.1, 0.59765625, ((0, 2),))
    return dict(grad_out=grad_out, saved_hidden=saved_hidden, routes=routes, scores=scores, down_weight=down_weight, router=router)


def slot_rows(route_ids, n_experts, per_block, capacity):
    flat_routes = route_ids.reshape(-1)
    entries = flat_routes.shape[0]
    n_blocks = entries // per_block
    onehot = (flat_routes[:, None] == jnp.arange(n_experts, dtype=jnp.int32)[None, :]).astype(jnp.int32)
    running = jnp.cumsum(onehot.reshape(n_blocks, per_block, n_experts), axis=1).astype(jnp.int32)
    running = running.reshape(entries, n_experts)
    slot_index = jnp.sum(running * onehot, axis=1).astype(jnp.int32) - 1
    block_index = jnp.arange(entries, dtype=jnp.int32) // per_block
    row_index = (block_index * capacity + slot_index).astype(jnp.int32)
    source = jnp.full((n_experts, n_blocks * capacity), entries, jnp.int32)
    source = source.at[flat_routes, row_index].set(jnp.arange(entries, dtype=jnp.int32))
    return flat_routes, row_index, source


def section_pass(grad_rows, hidden_rows, route_ids, score_rows, down_all, router_rows):
    n_tokens, n_routes = route_ids.shape
    n_experts = router_rows.shape[0]
    entries = n_tokens * n_routes
    flat_routes, row_index, source = slot_rows(route_ids, n_experts, TOK_DEV * n_routes, CAP)
    score_total = jnp.sum(score_rows, axis=1, keepdims=True)
    weights = score_rows / score_total
    weights_low = weights.astype(jnp.bfloat16).reshape(-1)
    hidden_flat = hidden_rows.reshape(entries, hidden_rows.shape[2])

    def one_expert(operands):
        slot_source, expert_down = operands
        filled = slot_source < entries
        safe_index = jnp.minimum(slot_source, entries - 1)
        grad_in = jnp.where(filled[:, None], grad_rows[safe_index // n_routes], jnp.zeros((), jnp.bfloat16))
        hidden_in = jnp.where(filled[:, None], hidden_flat[safe_index], jnp.zeros((), jnp.bfloat16))
        weight_in = jnp.where(filled, weights_low[safe_index], jnp.zeros((), jnp.bfloat16))
        projected = lax.dot_general(grad_in, expert_down, (((1,), (1,)), ((), ())), preferred_element_type=jnp.float32)
        derivs = jnp.sum(projected * hidden_in.astype(jnp.float32), axis=1)
        scaled = (weight_in.astype(jnp.float32)[:, None] * grad_in.astype(jnp.float32)).astype(jnp.bfloat16)
        weight_grads = lax.dot_general(hidden_in, scaled, (((0,), (0,)), ((), ())), preferred_element_type=jnp.float32)
        return weight_grads.astype(jnp.bfloat16), derivs

    weight_grads, derivs = lax.map(one_expert, (source, down_all))
    derivs_home = derivs[flat_routes, row_index].reshape(n_tokens, n_routes)
    center = jnp.sum(weights * derivs_home, axis=1, keepdims=True)
    logit_grad = score_rows * (1.0 - score_rows) / score_total * (derivs_home - center)
    expert_ids = jnp.arange(n_experts, dtype=jnp.int32)
    dense_grad = jnp.sum(jnp.where(route_ids[:, :, None] == expert_ids[None, None, :], logit_grad[:, :, None], 0.0), axis=1)
    input_grad = grad_rows.astype(jnp.float32) + jnp.dot(dense_grad, router_rows.astype(jnp.float32), precision=lax.Precision.HIGHEST)
    return weight_grads, input_grad.astype(jnp.bfloat16)


def reference(grad_out, saved_hidden, routes, scores, down_weight, router):
    weight_list = []
    input_list = []
    for section_index in range(SECTIONS):
        weight_grads, input_grad = section_pass(grad_out[section_index], saved_hidden[section_index], routes[section_index], scores[section_index], down_weight[section_index], router[section_index])
        weight_list.append(weight_grads)
        input_list.append(input_grad)
    handed = jnp.roll(jnp.stack(input_list), -1, axis=0)
    return jnp.stack(weight_list), handed
```

```python
import functools
import math

import jax
import jax.numpy as jnp
from jax import lax
from jax.experimental import pallas as pl
from jax.experimental.pallas import tpu as pltpu
from jax.sharding import PartitionSpec as P

META = 8
BF, F32 = jnp.bfloat16, jnp.float32


def iota(shape, dim):
    return lax.broadcasted_iota(jnp.int32, shape, dim)


def dot(a, b, ca, cb):
    return lax.dot_general(a, b, (((ca,), (cb,)), ((), ())), preferred_element_type=F32)


def exchange(array, offset):
    size = lax.axis_size("expert")
    return lax.ppermute(array, "expert", [(i, i ^ offset) for i in range(size)])


def earlier_count(mask):
    width = mask.shape[1]
    upper = (iota((width, width), 0) < iota((width, width), 1)).astype(F32).astype(BF)
    return dot(mask.astype(BF), upper, 1, 0)


def pack_kernel(n_experts, capacity, n_routes, group, routes_ref, weight_ref, hidden_ref, out_ref):
    entries = routes_ref.shape[1]
    n_tokens = entries // n_routes
    step = pl.program_id(0)
    routes = routes_ref[...]
    named = (routes == iota((n_experts, entries), 0)).astype(F32)
    spread = (iota((n_tokens, entries), 1) // n_routes == iota((n_tokens, entries), 0)).astype(F32).astype(BF)
    mask = dot(named.astype(BF), spread, 1, 1)
    rank = dot(earlier_count(mask).astype(BF), spread, 1, 0)
    place = jnp.sum(named * rank, axis=0, keepdims=True).astype(jnp.int32) + routes * capacity
    rows = group * capacity
    slots = iota((rows, entries), 0) + step * rows
    select = jnp.where(slots == place, weight_ref[...], 0.0).astype(BF)
    picked = dot(select, hidden_ref[...], 1, 0)
    meta_row = iota((META, n_tokens), 0) == 0
    for i in range(group):
        out_ref[i, 0:capacity, :] = picked[i * capacity : (i + 1) * capacity].astype(BF)
        out_ref[i, capacity : capacity + META, :] = jnp.zeros((META, hidden_ref.shape[1]), BF)
        own = iota((n_experts, n_tokens), 0) == step * group + i
        row = jnp.sum(jnp.where(own, mask, 0.0), axis=0, keepdims=True)
        out_ref[i, capacity : capacity + META, 0:n_tokens] = jnp.where(meta_row, row, 0.0).astype(BF)


def pack(routes_row, weight_row, hidden, n_experts, capacity, n_routes):
    entries, width = hidden.shape
    group = 4
    return pl.pallas_call(
        functools.partial(pack_kernel, n_experts, capacity, n_routes, group),
        grid=(n_experts // group,),
        in_specs=[
            pl.BlockSpec((1, entries), lambda i: (0, 0)),
            pl.BlockSpec((1, entries), lambda i: (0, 0)),
            pl.BlockSpec((entries, width), lambda i: (0, 0)),
        ],
        out_specs=pl.BlockSpec((group, capacity + META, width), lambda i: (i, 0, 0)),
        out_shape=jax.ShapeDtypeStruct((n_experts, capacity + META, width), BF),
        cost_estimate=pl.CostEstimate(
            flops=2 * n_experts * capacity * entries * width,
            bytes_accessed=2 * (entries + n_experts * capacity) * width,
            transcendentals=0,
        ),
        name="pack",
    )(routes_row, weight_row, hidden)


def expert_kernel(layout, capacity, steps, src_ref, *refs):
    n_pieces = sum(layout)
    n_blocks = len(layout)
    pieces = refs[:n_pieces]
    hiddens = refs[n_pieces : n_pieces + n_blocks]
    down_ref, slots_ref, rows_ref, derivs_ref, proj_ref, pick_ref = refs[n_pieces + n_blocks :]
    step = pl.program_id(0)
    n_tokens = derivs_ref.shape[1]

    @pl.when(step == 0)
    def _():
        masks = jnp.concatenate(
            [h[0, capacity : capacity + META, 0:n_tokens].astype(F32)[0:1] for h in hiddens], axis=0
        )
        ranks = earlier_count(masks).astype(jnp.int32)
        for j in range(n_blocks):
            hit = (iota((capacity, n_tokens), 0) == ranks[j : j + 1]) & (masks[j : j + 1] > 0.5)
            pick_ref[j] = hit.astype(F32)
        rows_ref[...] = jnp.concatenate(
            [h[0, 0:capacity, :].astype(F32) for h in hiddens], axis=0
        ).astype(BF)

    picked, at = [], 0
    for j, count in enumerate(layout):
        block = jnp.concatenate([p[...] for p in pieces[at : at + count]], axis=0)
        at += count
        picked.append(dot(pick_ref[j].astype(BF), block, 1, 0))
    slots = jnp.concatenate(picked, axis=0).astype(BF)
    slots_ref[...] = slots
    part = dot(slots, down_ref[...], 1, 1)

    @pl.when(step == 0)
    def _():
        proj_ref[...] = part

    @pl.when(step > 0)
    def _():
        proj_ref[...] += part

    @pl.when(step == steps - 1)
    def _():
        derivs = jnp.sum(proj_ref[...] * rows_ref[...].astype(F32), axis=1, keepdims=True)
        for j in range(n_blocks):
            own = derivs[j * capacity : (j + 1) * capacity]
            derivs_ref[j : j + 1, :] = jnp.sum(pick_ref[j] * own, axis=0, keepdims=True)


def expert_pass(blocks, sources, hidden_in, down, capacity):
    layout = tuple(len(b) for b in blocks)
    pieces = [p for b in blocks for p in b]
    n_blocks = len(blocks)
    n_tokens = sum(p.shape[0] for p in blocks[0])
    width, model = down.shape
    steps = 4
    cols = model // steps
    rows = n_blocks * capacity
    in_specs = [pl.BlockSpec((p.shape[0], cols), lambda i, s: (0, i)) for p in pieces]
    for j in range(n_blocks):
        in_specs.append(
            pl.BlockSpec((1, capacity + META, width), functools.partial(lambda j, i, s: (s[j], 0, 0), j))
        )
    in_specs.append(pl.BlockSpec((width, cols), lambda i, s: (0, i)))
    return pl.pallas_call(
        functools.partial(expert_kernel, layout, capacity, steps),
        grid_spec=pltpu.PrefetchScalarGridSpec(
            num_scalar_prefetch=1,
            grid=(steps,),
            in_specs=in_specs,
            out_specs=[
                pl.BlockSpec((rows, cols), lambda i, s: (0, i)),
                pl.BlockSpec((rows, width), lambda i, s: (0, 0)),
                pl.BlockSpec((n_blocks, n_tokens), lambda i, s: (0, 0)),
            ],
            scratch_shapes=[
                pltpu.VMEM((rows, width), F32),
                pltpu.VMEM((n_blocks, capacity, n_tokens), F32),
            ],
        ),
        out_shape=[
            jax.ShapeDtypeStruct((rows, model), BF),
            jax.ShapeDtypeStruct((rows, width), BF),
            jax.ShapeDtypeStruct((n_blocks, n_tokens), F32),
        ],
        cost_estimate=pl.CostEstimate(
            flops=2 * rows * model * (width + n_tokens),
            bytes_accessed=2 * (n_blocks * n_tokens * model + rows * model + width * model + 2 * rows * width),
            transcendentals=0,
        ),
        name="expert",
    )(sources, *pieces, *([hidden_in] * n_blocks), down)


def home_kernel(derivs_ref, routes_ref, scores_ref, router_ref, grad_ref, out_ref):
    n_experts, n_tokens = derivs_ref.shape
    n_routes = routes_ref.shape[0]
    score = jnp.zeros((n_experts, n_tokens), F32)
    named = jnp.zeros((n_experts, n_tokens), F32)
    for k in range(n_routes):
        hit = routes_ref[k : k + 1, :] == iota((n_experts, n_tokens), 0)
        score = jnp.where(hit, scores_ref[k : k + 1, :], score)
        named = jnp.where(hit, 1.0, named)
    total = jnp.sum(scores_ref[...], axis=0, keepdims=True)
    weight = score / total
    low = jnp.where(named > 0.5, weight.astype(BF).astype(F32), 1.0)
    weighted = jnp.where(named > 0.5, derivs_ref[...] * (weight / low), 0.0)
    center = jnp.sum(weighted, axis=0, keepdims=True)
    logit = named * (1.0 - score) * (weighted - weight * center)
    high = logit.astype(BF)
    rest = logit - high.astype(F32)
    middle = rest.astype(BF)
    last = (rest - middle.astype(F32)).astype(BF)
    router = router_ref[...]
    added = dot(high, router, 0, 0) + (dot(middle, router, 0, 0) + dot(last, router, 0, 0))
    out_ref[...] = (grad_ref[...].astype(F32) + added).astype(BF)


def home(derivs, routes_t, scores_t, router, grad):
    n_experts, n_tokens = derivs.shape
    n_routes = routes_t.shape[0]
    model = grad.shape[1]
    steps = 4
    cols = model // steps
    return pl.pallas_call(
        home_kernel,
        grid=(steps,),
        in_specs=[
            pl.BlockSpec((n_experts, n_tokens), lambda i: (0, 0)),
            pl.BlockSpec((n_routes, n_tokens), lambda i: (0, 0)),
            pl.BlockSpec((n_routes, n_tokens), lambda i: (0, 0)),
            pl.BlockSpec((n_experts, cols), lambda i: (0, i)),
            pl.BlockSpec((n_tokens, cols), lambda i: (0, i)),
        ],
        out_specs=pl.BlockSpec((n_tokens, cols), lambda i: (0, i)),
        out_shape=jax.ShapeDtypeStruct((n_tokens, model), BF),
        cost_estimate=pl.CostEstimate(
            flops=6 * n_experts * n_tokens * model, bytes_accessed=4 * n_tokens * model, transcendentals=0
        ),
        name="home",
    )(derivs, routes_t, scores_t, router, grad)


def factors(size):
    far = 4 if size % 4 == 0 else 1
    side = math.isqrt(size // far)
    return (far, side) if far * side * side == size else (size, 1)


def gathered(grad, size):
    far, side = factors(size)
    plane = side * side
    half = grad.shape[0] // 2
    bases = [grad] + [exchange(grad, r * plane) for r in range(1, far)]
    chunks = []
    for r, base in enumerate(bases):
        along_x = {i: exchange(base, i) for i in range(1, side)}
        along_y = {j: exchange(base, j * side) for j in range(1, side)}
        blocks, offsets = [(base,)], [r * plane]
        for i in range(1, side):
            blocks.append((along_x[i],))
            offsets.append(r * plane + i)
        for j in range(1, side):
            blocks.append((along_y[j],))
            offsets.append(r * plane + j * side)
        for i in range(1, side):
            for j in range(1, side):
                blocks.append((exchange(along_y[j][:half], i), exchange(along_x[i][half:], j * side)))
                offsets.append(r * plane + j * side + i)
        chunks.append((blocks, offsets))
    return chunks


def body(grad_out, saved_hidden, routes, scores, down_weight, router):
    grad_rows = grad_out[0]
    hidden_rows = saved_hidden[0]
    route_ids = routes[0]
    score_rows = scores[0]
    down = down_weight[0, 0]
    router_rows = router[0]
    n_tokens, n_routes, hidden_width = hidden_rows.shape
    n_experts = router_rows.shape[0]
    capacity = 3 * n_tokens * n_routes // (2 * n_experts)
    entries = n_tokens * n_routes
    me = lax.axis_index("expert")

    chunks = gathered(grad_rows, n_experts)
    weights = score_rows / jnp.sum(score_rows, axis=1, keepdims=True)
    packed = pack(
        route_ids.reshape(1, entries),
        weights.reshape(1, entries),
        hidden_rows.reshape(entries, hidden_width),
        n_experts,
        capacity,
        n_routes,
    )
    hidden_in = lax.all_to_all(packed, "expert", split_axis=0, concat_axis=0, tiled=True)

    total, derivs, order = None, [], []
    for blocks, offsets in chunks:
        sources = me ^ jnp.array(offsets, jnp.int32)
        slots, rows, part = expert_pass(blocks, sources, hidden_in, down, capacity)
        derivs.append(part)
        order += offsets
        product = lax.dot_general(rows, slots, (((0,), (0,)), ((), ())), preferred_element_type=F32)
        total = product if total is None else total + product
    by_offset = jnp.concatenate(derivs, axis=0)
    back = jnp.array([order.index(q) for q in range(n_experts)], jnp.int32)
    by_source = by_offset[back[jnp.arange(n_experts, dtype=jnp.int32) ^ me]]
    derivs_home = lax.all_to_all(
        by_source[:, None, :], "expert", split_axis=0, concat_axis=0, tiled=True
    ).reshape(n_experts, n_tokens)
    handed = home(derivs_home, route_ids.T, score_rows.T, router_rows, grad_rows)
    size = lax.axis_size("section")
    handed = lax.ppermute(handed, "section", [(i, (i - 1) % size) for i in range(size)])
    return (total.astype(BF)[None, None], handed[None])


def solution(mesh):
    return jax.shard_map(
        body,
        mesh=mesh,
        in_specs=(
            P("section", "expert", None),
            P("section", "expert", None, None),
            P("section", "expert", None),
            P("section", "expert", None),
            P("section", "expert", None, None),
            P("section", None, None),
        ),
        out_specs=(P("section", "expert", None, None), P("section", "expert", None)),
        check_vma=False,
    )
```

```python
import functools
import math

import jax
import jax.numpy as jnp
from jax import lax
from jax.experimental import pallas as pl
from jax.experimental.pallas import tpu as pltpu
from jax.sharding import PartitionSpec as P


META = 8
BF, F32 = jnp.bfloat16, jnp.float32


def iota(shape, dim):
    return lax.broadcasted_iota(jnp.int32, shape, dim)


def dot(a, b, ca, cb):
    return lax.dot_general(a, b, (((ca,), (cb,)), ((), ())), preferred_element_type=F32)


def send(array, pairs):
    return lax.ppermute(array, "expert", pairs)


def exchange(array, offset):
    size = lax.axis_size("expert")
    return send(array, [(i, i ^ offset) for i in range(size)])


def earlier_count(mask):
    width = mask.shape[1]
    upper = (iota((width, width), 0) < iota((width, width), 1)).astype(F32).astype(BF)
    return dot(mask.astype(BF), upper, 1, 0)


def pack_kernel(n_experts, capacity, n_routes, group, routes_ref, weight_ref, hidden_ref, out_ref):
    entries = routes_ref.shape[1]
    n_tokens = entries // n_routes
    step = pl.program_id(0)
    routes = routes_ref[...]
    named = (routes == iota((n_experts, entries), 0)).astype(F32)
    spread = (iota((n_tokens, entries), 1) // n_routes == iota((n_tokens, entries), 0)).astype(F32).astype(BF)
    mask = dot(named.astype(BF), spread, 1, 1)
    rank = dot(earlier_count(mask).astype(BF), spread, 1, 0)
    place = jnp.sum(named * rank, axis=0, keepdims=True).astype(jnp.int32) + routes * capacity
    rows = group * capacity
    slots = iota((rows, entries), 0) + step * rows
    select = jnp.where(slots == place, weight_ref[...], 0.0).astype(BF)
    picked = dot(select, hidden_ref[...], 1, 0)
    meta_row = iota((META, n_tokens), 0) == 0
    for i in range(group):
        out_ref[i, 0:capacity, :] = picked[i * capacity : (i + 1) * capacity].astype(BF)
        out_ref[i, capacity : capacity + META, :] = jnp.zeros((META, hidden_ref.shape[1]), BF)
        own = iota((n_experts, n_tokens), 0) == step * group + i
        row = jnp.sum(jnp.where(own, mask, 0.0), axis=0, keepdims=True)
        out_ref[i, capacity : capacity + META, 0:n_tokens] = jnp.where(meta_row, row, 0.0).astype(BF)


def pack(routes_row, weight_row, hidden, n_experts, capacity, n_routes):
    entries, width = hidden.shape
    group = 4
    return pl.pallas_call(
        functools.partial(pack_kernel, n_experts, capacity, n_routes, group),
        grid=(n_experts // group,),
        in_specs=[
            pl.BlockSpec((1, entries), lambda i: (0, 0)),
            pl.BlockSpec((1, entries), lambda i: (0, 0)),
            pl.BlockSpec((entries, width), lambda i: (0, 0)),
        ],
        out_specs=pl.BlockSpec((group, capacity + META, width), lambda i: (i, 0, 0)),
        out_shape=jax.ShapeDtypeStruct((n_experts, capacity + META, width), BF),
        cost_estimate=pl.CostEstimate(
            flops=2 * n_experts * capacity * entries * width,
            bytes_accessed=2 * (entries + n_experts * capacity) * width,
            transcendentals=0,
        ),
        name="pack",
    )(routes_row, weight_row, hidden)


def spread_kernel(capacity, group, src_ref, *refs):
    hiddens, (dense_ref, turned_ref) = refs[:group], refs[group:]
    n_tokens = dense_ref.shape[0] // group
    masks = jnp.concatenate(
        [h[0, capacity : capacity + META, 0:n_tokens].astype(F32)[0:1] for h in hiddens], axis=0
    )
    ranks = earlier_count(masks).astype(jnp.int32)
    for j in range(group):
        hit = (iota((capacity, n_tokens), 0) == ranks[j : j + 1]) & (masks[j : j + 1] > 0.5)
        dense = dot(hit.astype(F32).astype(BF), hiddens[j][0, 0:capacity, :], 0, 0).astype(BF)
        dense_ref[j * n_tokens : (j + 1) * n_tokens, :] = dense
        turned_ref[:, j * n_tokens : (j + 1) * n_tokens] = dense.T


def spread(sources, hidden_in, capacity, n_tokens):
    count = sources.shape[0]
    width = hidden_in.shape[2]
    group = 4 if count % 4 == 0 else 1
    return pl.pallas_call(
        functools.partial(spread_kernel, capacity, group),
        grid_spec=pltpu.PrefetchScalarGridSpec(
            num_scalar_prefetch=1,
            grid=(count // group,),
            in_specs=[
                pl.BlockSpec(
                    (1, capacity + META, width),
                    functools.partial(lambda j, i, s: (s[i * group + j], 0, 0), j),
                )
                for j in range(group)
            ],
            out_specs=[
                pl.BlockSpec((group * n_tokens, width), lambda i, s: (i, 0)),
                pl.BlockSpec((width, group * n_tokens), lambda i, s: (0, i)),
            ],
        ),
        out_shape=[
            jax.ShapeDtypeStruct((count * n_tokens, width), BF),
            jax.ShapeDtypeStruct((width, count * n_tokens), BF),
        ],
        cost_estimate=pl.CostEstimate(
            flops=2 * count * n_tokens * capacity * width,
            bytes_accessed=6 * count * n_tokens * width,
            transcendentals=0,
        ),
        name="spread",
    )(sources, *([hidden_in] * group))


def n_steps(n_blocks):
    return 2 if n_blocks <= 4 else 4 if n_blocks <= 16 else 8


def project_step(blocks, down_ref, proj_ref):
    part = dot(jnp.concatenate([b[...] for b in blocks], axis=0), down_ref[...], 1, 1)

    @pl.when(pl.program_id(0) == 0)
    def _():
        proj_ref[...] = part

    @pl.when(pl.program_id(0) > 0)
    def _():
        proj_ref[...] += part


def project_kernel(*refs):
    project_step(refs[:-2], *refs[-2:])


def project(blocks, down):
    n_tokens, model = blocks[0].shape
    width = down.shape[0]
    steps = n_steps(len(blocks))
    cols = model // steps
    rows = len(blocks) * n_tokens
    return pl.pallas_call(
        project_kernel,
        grid=(steps,),
        in_specs=[pl.BlockSpec((n_tokens, cols), lambda i: (0, i)) for _ in blocks]
        + [pl.BlockSpec((width, cols), lambda i: (0, i))],
        out_specs=pl.BlockSpec((rows, width), lambda i: (0, 0)),
        out_shape=jax.ShapeDtypeStruct((rows, width), F32),
        cost_estimate=pl.CostEstimate(
            flops=2 * rows * model * width,
            bytes_accessed=2 * model * (rows + width) + 4 * rows * width,
            transcendentals=0,
        ),
        name="project",
    )(*blocks, down)


def expert_kernel(n_blocks, n_early, steps, src_ref, *refs):
    blocks, (down_ref, hidden_ref), rest = refs[:n_blocks], refs[n_blocks : n_blocks + 2], refs[n_blocks + 2 :]
    early_ref, derivs_ref, proj_ref = rest if n_early else (None, *rest)
    n_tokens = blocks[0].shape[0]
    project_step(blocks, down_ref, proj_ref)
    diagonal = iota((n_tokens, n_tokens), 0) == iota((n_tokens, n_tokens), 1)

    def reduce(values_ref, at, j):
        values = values_ref[(j - at) * n_tokens : (j - at + 1) * n_tokens, :]
        hidden = hidden_ref[j * n_tokens : (j + 1) * n_tokens, :].astype(F32)
        column = jnp.sum(values * hidden, axis=1, keepdims=True)
        derivs_ref[src_ref[j], :, :] = jnp.sum(jnp.where(diagonal, column, 0.0), axis=0, keepdims=True)

    @pl.when(pl.program_id(0) == steps - 1)
    def _():
        for j in range(n_early):
            reduce(early_ref, 0, j)
        for j in range(n_early, n_early + n_blocks):
            reduce(proj_ref, n_early, j)


def expert_pass(blocks, sources, hidden, down, earlier=None, early=None):
    n_blocks = len(blocks)
    n_tokens, model = blocks[0].shape
    width = down.shape[0]
    n_early = 0 if early is None else early.shape[0] // n_tokens
    steps = n_steps(n_blocks)
    cols = model // steps
    rows = n_blocks * n_tokens
    in_specs = [pl.BlockSpec((n_tokens, cols), lambda i, s: (0, i)) for _ in blocks]
    in_specs.append(pl.BlockSpec((width, cols), lambda i, s: (0, i)))
    in_specs.append(pl.BlockSpec(hidden.shape, lambda i, s: (0, 0)))
    operands = [*blocks, down, hidden]
    if n_early:
        in_specs.append(pl.BlockSpec(early.shape, lambda i, s: (0, 0)))
        operands.append(early)
    n_experts = earlier.shape[0]
    kernel = functools.partial(expert_kernel, n_blocks, n_early, steps)

    def with_earlier(src_ref, earlier_ref, *refs):
        @pl.when(pl.program_id(0) == 0)
        def _():
            refs[-2][...] = earlier_ref[...]

        kernel(src_ref, *refs)

    whole = pl.BlockSpec((n_experts, 1, n_tokens), lambda i, s: (0, 0, 0))
    return pl.pallas_call(
        with_earlier,
        grid_spec=pltpu.PrefetchScalarGridSpec(
            num_scalar_prefetch=1,
            grid=(steps,),
            in_specs=[whole] + in_specs,
            out_specs=whole,
            scratch_shapes=[pltpu.VMEM((rows, width), F32)],
        ),
        out_shape=jax.ShapeDtypeStruct((n_experts, 1, n_tokens), F32),
        cost_estimate=pl.CostEstimate(
            flops=2 * rows * model * width,
            bytes_accessed=2 * model * (rows + width) + 6 * (n_early + n_blocks) * n_tokens * width,
            transcendentals=0,
        ),
        name="expert",
    )(sources, earlier, *operands)


def weight_kernel(counts, has_earlier, *refs):
    n_groups, out_ref = len(counts), refs[-1]
    at, part = n_groups, None
    for g, count in enumerate(counts):
        block = jnp.concatenate([b[...] for b in refs[at : at + count]], axis=0)
        at += count
        product = dot(refs[g][...], block, 1, 0)
        part = product if part is None else part + product
    if has_earlier:
        part += refs[at][...]
    out_ref[...] = part.astype(out_ref.dtype)


def weight_pass(turned, groups, dtype, part=0, parts=1, steps=4, earlier=None, into=None):
    width = turned[0].shape[0]
    n_tokens, model = groups[0][0].shape
    cols = model // (parts * steps)
    start = part * steps
    blocks = [b for g in groups for b in g]
    column = lambda i: (0, start + i)
    operands = [*turned, *blocks]
    in_specs = [pl.BlockSpec(t.shape, lambda i: (0, 0)) for t in turned]
    in_specs += [pl.BlockSpec((n_tokens, cols), column) for _ in blocks]
    if earlier is not None:
        operands.append(earlier)
        in_specs.append(pl.BlockSpec((width, cols), column))
    aliases = {}
    if into is not None:
        aliases = {len(operands): 0}
        operands.append(into)
        in_specs.append(pl.BlockSpec(memory_space=pl.ANY))
    depth = len(blocks) * n_tokens
    return pl.pallas_call(
        functools.partial(weight_kernel, tuple(len(g) for g in groups), earlier is not None),
        grid=(steps,),
        in_specs=in_specs,
        out_specs=pl.BlockSpec((width, cols), column),
        out_shape=jax.ShapeDtypeStruct((width, model), dtype),
        input_output_aliases=aliases,
        cost_estimate=pl.CostEstimate(
            flops=2 * depth * width * model // parts,
            bytes_accessed=(2 * depth + 6 * width) * model // parts,
            transcendentals=0,
        ),
        name="weight",
    )(*operands)


def home_kernel(derivs_ref, routes_ref, scores_ref, router_ref, grad_ref, out_ref):
    n_experts, n_tokens = derivs_ref.shape
    n_routes = routes_ref.shape[0]
    score = jnp.zeros((n_experts, n_tokens), F32)
    named = jnp.zeros((n_experts, n_tokens), F32)
    for k in range(n_routes):
        hit = routes_ref[k : k + 1, :] == iota((n_experts, n_tokens), 0)
        score = jnp.where(hit, scores_ref[k : k + 1, :], score)
        named = jnp.where(hit, 1.0, named)
    total = jnp.sum(scores_ref[...], axis=0, keepdims=True)
    weight = score / total
    low = jnp.where(named > 0.5, weight.astype(BF).astype(F32), 1.0)
    weighted = jnp.where(named > 0.5, derivs_ref[...] * (weight / low), 0.0)
    center = jnp.sum(weighted, axis=0, keepdims=True)
    logit = named * (1.0 - score) * (weighted - weight * center)
    high = logit.astype(BF)
    rest = logit - high.astype(F32)
    middle = rest.astype(BF)
    last = (rest - middle.astype(F32)).astype(BF)
    router = router_ref[...]
    added = dot(high, router, 0, 0) + (dot(middle, router, 0, 0) + dot(last, router, 0, 0))
    out_ref[...] = (grad_ref[...].astype(F32) + added).astype(BF)


def home(derivs, routes_t, scores_t, router, grad):
    n_experts, n_tokens = derivs.shape
    n_routes = routes_t.shape[0]
    model = grad.shape[1]
    steps = 4
    cols = model // steps
    return pl.pallas_call(
        home_kernel,
        grid=(steps,),
        in_specs=[
            pl.BlockSpec((n_experts, n_tokens), lambda i: (0, 0)),
            pl.BlockSpec((n_routes, n_tokens), lambda i: (0, 0)),
            pl.BlockSpec((n_routes, n_tokens), lambda i: (0, 0)),
            pl.BlockSpec((n_experts, cols), lambda i: (0, i)),
            pl.BlockSpec((n_tokens, cols), lambda i: (0, i)),
        ],
        out_specs=pl.BlockSpec((n_tokens, cols), lambda i: (0, i)),
        out_shape=jax.ShapeDtypeStruct((n_tokens, model), BF),
        cost_estimate=pl.CostEstimate(
            flops=6 * n_experts * n_tokens * model, bytes_accessed=4 * n_tokens * model, transcendentals=0
        ),
        name="home",
    )(derivs, routes_t, scores_t, router, grad)


def factors(size):
    far = 4 if size % 4 == 0 else 1
    side = math.isqrt(size // far)
    return (far, side) if far * side * side == size else (size, 1)


def gather_blocks(grad, size, me):
    far, side = factors(size)
    plane = side * side
    rest = range(1, side)
    if far == 1:
        blocks = [(grad, jnp.int32(0))] + [(exchange(grad, i), jnp.int32(i)) for i in range(1, size)]
        return [[], [], blocks]
    z = (me // plane) % far
    inner = (z == 1) | (z == 2)
    across = [(i, i ^ (3 * plane)) for i in range(size) if (i // plane) % far in (1, 2)]
    outward = [(i, i ^ plane) for i in range(size) if (i // plane) % far in (1, 2)]
    near = exchange(grad, plane)
    own = send(grad, across)
    passed = send(near, across)
    own_out = send(own, outward)
    passed_out = send(passed, outward)
    two, three = jnp.int32(2 * plane), jnp.int32(3 * plane)
    bases = [
        (grad, jnp.int32(0)),
        (near, jnp.int32(plane)),
        (jnp.where(inner, own, own_out), jnp.where(inner, three, two)),
        (jnp.where(inner, passed, passed_out), jnp.where(inner, two, three)),
    ]
    straight, corner = [], []
    for r, (base, offset) in enumerate(bases):
        along_x = {i: exchange(base, i) for i in rest}
        along_y = {j: exchange(base, j * side) for j in rest}
        straight.append(
            [(along_x[i], offset ^ i) for i in rest] + [(along_y[j], offset ^ (j * side)) for j in rest]
        )
        corner.append(
            [
                (
                    exchange(along_y[j], i)
                    if r % 2 == 0
                    else exchange(along_x[i], j * side),
                    offset ^ (j * side + i),
                )
                for i in rest
                for j in rest
            ]
        )
    return [
        [bases[0]] + straight[0] + corner[0] + [bases[1]] + straight[1] + [bases[2]],
        [bases[3]] + straight[2] + corner[1],
        straight[3] + corner[2] + corner[3],
    ]


def body(grad_out, saved_hidden, routes, scores, down_weight, router):
    grad_rows = grad_out[0]
    hidden_rows = saved_hidden[0]
    route_ids = routes[0]
    score_rows = scores[0]
    down = down_weight[0, 0]
    router_rows = router[0]
    n_tokens, n_routes, hidden_width = hidden_rows.shape
    n_experts = router_rows.shape[0]
    capacity = 3 * n_tokens * n_routes // (2 * n_experts)
    entries = n_tokens * n_routes
    me = lax.axis_index("expert")

    group_a, group_b, group_c = gather_blocks(grad_rows, n_experts, me)
    weights = score_rows / jnp.sum(score_rows, axis=1, keepdims=True)
    packed = pack(
        route_ids.reshape(1, entries),
        weights.reshape(1, entries),
        hidden_rows.reshape(entries, hidden_width),
        n_experts,
        capacity,
        n_routes,
    )
    hidden_in = lax.all_to_all(packed, "expert", split_axis=0, concat_axis=0, tiled=True)

    arrays = lambda group: [b for b, _ in group]
    sources = lambda group: me ^ jnp.stack([o for _, o in group])
    derivs = jnp.zeros((n_experts, 1, n_tokens), F32)
    group_ab = group_a + group_b
    if group_ab:
        early = project(arrays(group_a), down)
        dense_ab, turned_ab = spread(sources(group_ab), hidden_in, capacity, n_tokens)
        derivs = expert_pass(arrays(group_b), sources(group_ab), dense_ab, down, derivs, early)
    dense_c, turned_c = spread(sources(group_c), hidden_in, capacity, n_tokens)
    derivs = expert_pass(arrays(group_c), sources(group_c), dense_c, down, derivs)
    derivs_home = lax.all_to_all(derivs, "expert", split_axis=0, concat_axis=0, tiled=True)
    handed = home(
        derivs_home.reshape(n_experts, n_tokens), route_ids.T, score_rows.T, router_rows, grad_rows
    )
    size = lax.axis_size("section")
    handed = lax.ppermute(handed, "section", [(i, (i - 1) % size) for i in range(size)])
    turned, groups, sums = [turned_c], [arrays(group_c)], None
    if group_ab and len(group_ab) < 32:
        sums = weight_pass([turned_ab], [arrays(group_ab)], F32)
    elif group_ab:
        turned, groups = [turned_ab, turned_c], [arrays(group_ab), arrays(group_c)]
    total, parts = None, 2
    for p in range(parts):
        steps = 2 if sums is not None else 8
        total = weight_pass(turned, groups, BF, p, parts, steps, sums, total)
    return (total[None, None], handed[None])


def solution(mesh):
    return jax.shard_map(
        body,
        mesh=mesh,
        in_specs=(
            P("section", "expert", None),
            P("section", "expert", None, None),
            P("section", "expert", None),
            P("section", "expert", None),
            P("section", "expert", None, None),
            P("section", None, None),
        ),
        out_specs=(P("section", "expert", None, None), P("section", "expert", None)),
        check_vma=False,
    )
```
